32 devices in a mesh: expert: 16 (over z, y, x), replica: 2 (over core).
Axes of the slice: x: 2, y: 2, z: 4, core: 2. Of those that a mesh axis runs over, the one named last changes fastest.
Arguments:
- a_tokens: bfloat16 [2048, 2048], P(('expert', 'replica')), may hold values from -6 to 6
- a_ids: int32 [2048, 6], P(('expert', 'replica')), may hold values from 0 to 15, all different within a row
- a_gates: float32 [2048, 6], P(('expert', 'replica')), may hold values from 0.05 to 0.6
- a_valid: int32 [2048], P(('expert', 'replica')), may hold values 0 or 1
- b_cot: bfloat16 [2048, 2048], P(('expert', 'replica')), may hold values from -0.86328125 to 0.86328125
- b_ids: int32 [2048, 6], P(('expert', 'replica')), may hold values from 0 to 15, all different within a row
- b_gates: float32 [2048, 6], P(('expert', 'replica')), may hold values from 0.05 to 0.6
- b_valid: int32 [2048], P(('expert', 'replica')), may hold values 0 or 1
- b_hidden: bfloat16 [16, 768, 704], P('expert', 'replica'), may hold values from -6 to 6
- w_gate: bfloat16 [16, 2048, 704], P('expert'), may hold values from -0.125 to 0.125
- w_up: bfloat16 [16, 2048, 704], P('expert'), may hold values from -0.125 to 0.125
- w_down: bfloat16 [16, 704, 2048], P('expert'), may hold values from -0.21875 to 0.21875
Outputs:
- a_out: bfloat16 [2048, 2048], P(('expert', 'replica'))
- grad_down: float32 [16, 704, 2048], P('expert', None, 'replica')
The draws below stay inside these ranges and needn't reach their ends.
Inputs may be any that keep to these rules, and one draw needn't show every extreme that they name: `a_ids`: each token names 6 different experts. `b_ids`: each token names 6 different experts.
All inputs are finite; a program needn't handle non-finite values. No bound on the sum of `a_valid` or of `b_valid` on one device may be relied on, other than what follows from the above.
Results may differ from the reference program's by a relative error of at most 0.012.
Values may be sent and summed in bfloat16 or wider, within the bound.
No kernel may reach another device: no remote copies, remote signals or barrier semaphores. Data moves between devices by JAX's collectives and lax.ppermute only.
A program may use at most 64 MiB of HBM per device.

```python
import math
from functools import partial
import jax
import jax.numpy as jnp
from jax import lax

D = 2048
FW = 704
TOP = 6
TOK_DEV = 64
EXPERTS = 16
CAP = 24
TOKENS = 2048
SLOTS = 768
N_EXPERT = 16
N_REPLICA = 2


def touch_ends(drawn, rng, smallest, top_value):
    longest = drawn.shape.index(max(drawn.shape))
    spots = []
    for shift in (0, 1):
        where = [jax.random.randint(jax.random.fold_in(rng, axis), (), 0, length) for axis, length in enumerate(drawn.shape)]
        where[longest] = (where[longest] + shift) % drawn.shape[longest]
        spots.append(tuple(where))
    return drawn.at[spots[0]].set(smallest).at[spots[1]].set(top_value)


def spiked(entries, stream_key, source, target, blocks, factor):
    owner, partner = [(jnp.arange(entries.shape[dim]) // (entries.shape[dim] // blocks)).reshape([-1 if axis == dim else 1 for axis in range(entries.ndim)]) for dim in (source, target)]
    chosen = jax.random.permutation(stream_key, blocks)[partner]
    strong = (owner == chosen) | (owner == (partner + blocks // 2) % blocks)
    return jnp.where(strong, factor * entries, entries)


def levels(stream_key, dims, split, least, largest):
    factor_of, own = 1.0, jax.random.fold_in(stream_key, 6)
    for dim, shards_of in split:
        steps = jnp.exp(jax.random.uniform(jax.random.fold_in(own, dim), (shards_of,), jnp.float32, least / len(split), largest / len(split)))
        factor_of = factor_of * jnp.repeat(steps, dims[dim] // shards_of).reshape([-1 if axis == dim else 1 for axis in range(len(dims))])
    return factor_of


def distinct(stream_key, rows, number_of, top, lift):
    sequence = jax.random.permutation(jax.random.fold_in(stream_key, 1), number_of)
    boost = sequence
    for power in range(3):
        boost = boost * boost // number_of
    boost = boost * lift // number_of
    tickets = jax.random.randint(jax.random.fold_in(stream_key, 2), (rows, number_of), 0, 4096) + boost
    fixed_rows = jax.random.permutation(jax.random.fold_in(stream_key, 3), rows)[jnp.arange(number_of) % rows]
    tickets = jnp.where(jnp.arange(rows)[:, None] == fixed_rows[None, :], 1 << 14, tickets)
    score = tickets * number_of + jnp.arange(number_of)
    return lax.top_k(score.astype(jnp.int32), top)[1].astype(jnp.int32)


def noise(own_key, extent, deviation, reach, cuts=(), kind=jnp.bfloat16):
    level = levels(own_key, extent, cuts, -0.22, 0.18) if cuts else 1.0
    entries = jax.random.normal(own_key, extent, jnp.float32) * deviation * level
    return jnp.minimum(jnp.maximum(entries, -reach), reach).astype(kind)


def bell_draw_with(own_key, extent, width, limit, split, heavy, kind=jnp.bfloat16):
    values = width * jax.random.normal(own_key, extent, jnp.float32)
    if split:
        values = values * levels(own_key, extent, split, -0.22, 0.18)
    return jnp.clip(spiked(values, jax.random.fold_in(own_key, 3), *heavy), -limit, limit).astype(kind)


def setup_inputs(seed: int = 0) -> dict:
    key_of = jax.random.split(jax.random.key(seed), 13)
    a_tokens = noise(key_of[0], (TOKENS, D), 1.0, 6.0, ((0, 32),))
    a_ids = distinct(key_of[1], TOKENS, EXPERTS, TOP, 3072)
    a_gates = jnp.clip(jnp.exp(math.log(0.6) - 2.4849067 * jax.random.uniform(key_of[2], (TOKENS, TOP), jnp.float32) ** levels(key_of[2], (TOKENS, TOP), ((0, 32),), -0.2, 0.2)), 0.05, 0.6)
    a_valid = touch_ends((jax.random.randint(key_of[3], (TOKENS,), 0, 8) < 7).astype(jnp.int32), jax.random.fold_in(key_of[3], 1), 0, 1)
    b_cot = bell_draw_with(key_of[4], (TOKENS, D), (4.0 / (N_REPLICA * TOK_DEV * TOP) ** 0.5), 0.86328125, ((0, 32),), (0, 1, 32, 2.75))
    b_ids = distinct(key_of[5], TOKENS, EXPERTS, TOP, 3072)
    b_gates = jnp.clip(jnp.exp(math.log(0.6) - 2.4849067 * jax.random.uniform(key_of[6], (TOKENS, TOP), jnp.float32) ** levels(key_of[6], (TOKENS, TOP), ((0, 32),), -0.2, 0.2)), 0.05, 0.6)
    b_valid = touch_ends((jax.random.randint(key_of[7], (TOKENS,), 0, 8) < 7).astype(jnp.int32), jax.random.fold_in(key_of[7], 1), 0, 1)
    b_hidden = noise(key_of[8], (EXPERTS, SLOTS, FW), 1.0, 6.0, ((0, 16), (1, 2)))
    w_gate = noise(key_of[9], (EXPERTS, D, FW), D ** -0.5, 0.125, ((0, 16),))
    w_up = noise(key_of[10], (EXPERTS, D, FW), D ** -0.5, 0.125, ((0, 16),))
    w_down = noise(key_of[11], (EXPERTS, FW, D), FW ** -0.5, 0.21875, ((0, 16),))
    return dict(a_tokens=a_tokens, a_ids=a_ids, a_gates=a_gates, a_valid=a_valid, b_cot=b_cot, b_ids=b_ids, b_gates=b_gates, b_valid=b_valid, b_hidden=b_hidden, w_gate=w_gate, w_up=w_up, w_down=w_down)


def slot_keys(expert_ids, valid_mask, experts, capacity):
    top_count = expert_ids.shape[1]
    flat_ids = expert_ids.reshape(-1)
    live = jnp.repeat(valid_mask, top_count) > 0
    onehot = ((flat_ids[:, None] == jnp.arange(experts, dtype=jnp.int32)[None, :]) & live[:, None]).astype(jnp.int32)
    earlier = jnp.cumsum(onehot, axis=0) - onehot
    position = lax.optimization_barrier(jnp.sum(earlier * onehot, axis=1))
    kept_mask = live & (position < capacity)
    return jnp.where(kept_mask, flat_ids * capacity + position, -1).astype(jnp.int32)

def gather_tokens(slot_key, tokens, experts, capacity):
    total = experts * capacity
    tok_count = tokens.shape[0]
    matches = jnp.arange(total, dtype=jnp.int32)[:, None] == slot_key[None, :]
    picker = jnp.any(matches.reshape(total, tok_count, -1), axis=2).astype(jnp.bfloat16)
    sent = jnp.dot(picker, tokens, preferred_element_type=jnp.float32).astype(jnp.bfloat16)
    return sent.reshape(experts, capacity, tokens.shape[1])

def gated_slots(slot_key, gate_values, cotangent, experts, capacity):
    total = experts * capacity
    tok_count = cotangent.shape[0]
    flat_gates = gate_values.reshape(-1)
    matches = jnp.arange(total, dtype=jnp.int32)[:, None] == slot_key[None, :]
    picker = jnp.any(matches.reshape(total, tok_count, -1), axis=2).astype(jnp.bfloat16)
    copied = jnp.dot(picker, cotangent, preferred_element_type=jnp.float32)
    slot_gate = lax.optimization_barrier(jnp.sum(jnp.where(matches, flat_gates[None, :], jnp.zeros_like(flat_gates)[None, :]), axis=1))
    slots = copied * slot_gate[:, None]
    return slots.astype(jnp.bfloat16).reshape(experts, capacity, cotangent.shape[1])

def combine_slots(slot_key, gate_values, returned):
    model_width = returned.shape[-1]
    flat_rows = returned.reshape(-1, model_width)
    picked = flat_rows[jnp.maximum(slot_key, 0)]
    flat_gates = gate_values.reshape(-1)
    scale = jnp.where(slot_key >= 0, flat_gates, jnp.zeros_like(flat_gates))
    summed = picked.astype(flat_gates.dtype) * scale[:, None]
    return lax.optimization_barrier(jnp.sum(summed.reshape(gate_values.shape[0], gate_values.shape[1], model_width), axis=1)).astype(jnp.bfloat16)

def expert_ffn(inputs, gate_weight, up_weight, down_weight):
    model_width = inputs.shape[-1]
    rows = inputs.reshape(-1, model_width)
    gate_proj = jnp.dot(rows, gate_weight, preferred_element_type=jnp.float32)
    up_proj = jnp.dot(rows, up_weight, preferred_element_type=jnp.float32)
    hidden = (jax.nn.silu(gate_proj) * up_proj).astype(jnp.bfloat16)
    result = jnp.dot(hidden, down_weight, preferred_element_type=jnp.float32).astype(jnp.bfloat16)
    return result.reshape(inputs.shape[:-1] + (down_weight.shape[1],))

def group_view(array):
    return jnp.swapaxes(array.reshape((N_EXPERT, N_REPLICA, TOK_DEV) + array.shape[1:]), 0, 1)

def reference(a_tokens, a_ids, a_gates, a_valid, b_cot, b_ids, b_gates, b_valid, b_hidden, w_gate, w_up, w_down):
    hidden_groups = jnp.swapaxes(b_hidden.reshape(EXPERTS, N_REPLICA, N_EXPERT * CAP, FW), 0, 1)
    pieces_all = (group_view(a_tokens), group_view(a_ids), group_view(a_gates), group_view(a_valid), group_view(b_cot), group_view(b_ids), group_view(b_gates), group_view(b_valid), hidden_groups)
    make_keys = partial(slot_keys, experts=EXPERTS, capacity=CAP)
    make_sends = partial(gather_tokens, experts=EXPERTS, capacity=CAP)
    make_slots = partial(gated_slots, experts=EXPERTS, capacity=CAP)

    def run_expert(item):
        return expert_ffn(item[0], item[1], item[2], item[3])

    def expert_grad(item):
        return jnp.dot(item[0].T, item[1], preferred_element_type=jnp.float32)

    def one_group(running, pieces):
        a_tok, a_id, a_gate, a_live, b_tan, b_id, b_gate, b_live, b_hid = pieces
        a_keys = jax.vmap(make_keys)(a_id, a_live)
        sends = jax.vmap(make_sends)(a_keys, a_tok)
        arriving = jnp.swapaxes(sends, 0, 1)
        outputs = lax.map(run_expert, (arriving, w_gate, w_up, w_down))
        returned = jnp.swapaxes(outputs, 0, 1)
        group_out = jax.vmap(combine_slots)(a_keys, a_gate, returned)
        b_keys = jax.vmap(make_keys)(b_id, b_live)
        slots = jax.vmap(make_slots)(b_keys, b_gate, b_tan)
        per_expert = jnp.swapaxes(slots, 0, 1).reshape(EXPERTS, N_EXPERT * CAP, D)
        partial_grad = lax.map(expert_grad, (b_hid, per_expert))
        rounded = lax.optimization_barrier(partial_grad.astype(jnp.bfloat16)).astype(jnp.float32)
        return (running + rounded, group_out)
    start = jnp.zeros((EXPERTS, FW, D), jnp.float32)
    gradient, outs = lax.scan(one_group, start, pieces_all)
    a_out = jnp.swapaxes(outs, 0, 1).reshape(-1, D)
    return (a_out, gradient)
```

```python
import jax
import jax.numpy as jnp
from jax import lax
from jax.sharding import PartitionSpec as P


def routing(ids, gates, valid, experts, capacity):
    eq = ids[:, :, None] == jnp.arange(experts, dtype=jnp.int32)[None, None, :]
    hit = jnp.any(eq, axis=1) & (valid > 0)[:, None]
    gate = jnp.sum(jnp.where(eq, gates[:, :, None], 0.0), axis=1)
    count = ids.shape[0]
    row = lax.broadcasted_iota(jnp.int32, (count, count), 0)
    col = lax.broadcasted_iota(jnp.int32, (count, count), 1)
    earlier = jnp.dot(
        (col < row).astype(jnp.bfloat16),
        hit.astype(jnp.bfloat16),
        preferred_element_type=jnp.float32,
    )
    slot = jnp.where(hit & (earlier < capacity), earlier, -1.0)
    return slot, gate


def pick_matrix(slot, capacity):
    at = jnp.arange(capacity, dtype=jnp.int32).astype(jnp.float32)
    return slot.T[:, None, :] == at[None, :, None]


def pick(slot, tokens, capacity):
    match = pick_matrix(slot, capacity)
    one = match.reshape(-1, tokens.shape[0]).astype(jnp.bfloat16)
    return jnp.dot(one, tokens, preferred_element_type=jnp.float32)


def pick_gated(slot, gate, cot, capacity):
    match = pick_matrix(slot, capacity)
    weight = jnp.sum(jnp.where(match, gate.T[:, None, :], 0.0), axis=2).reshape(-1)
    one = match.reshape(-1, cot.shape[0]).astype(jnp.bfloat16)
    copied = jnp.dot(one, cot, preferred_element_type=jnp.float32)
    return (copied * weight[:, None]).astype(jnp.bfloat16)


def combine(slot, gate, rows, capacity):
    at = jnp.arange(capacity, dtype=jnp.int32).astype(jnp.float32)
    coef = jnp.where(slot[:, :, None] == at[None, None, :], gate[:, :, None], 0.0)
    coef = coef.reshape(slot.shape[0], -1)
    high = lax.reduce_precision(coef, 8, 7)
    low = (coef - high).astype(jnp.bfloat16)
    high = high.astype(jnp.bfloat16)
    return jnp.dot(high, rows, preferred_element_type=jnp.float32) + jnp.dot(
        low, rows, preferred_element_type=jnp.float32
    )


def body(
    a_tokens,
    a_ids,
    a_gates,
    a_valid,
    b_cot,
    b_ids,
    b_gates,
    b_valid,
    b_hidden,
    w_gate,
    w_up,
    w_down,
):
    experts = lax.axis_size("expert")
    replicas = lax.axis_size("replica")
    half = experts // 2
    capacity = b_hidden.shape[1] // experts
    width = a_tokens.shape[1]
    count = a_tokens.shape[0]
    side = lax.axis_index("expert") // half
    across = [(e, (e + half) % experts) for e in range(experts)]
    groups = [[s * half + i for i in range(half)] for s in range(2)]

    def swap(x):
        return lax.ppermute(x, "expert", across)

    def spread(x):
        return lax.all_to_all(
            x, "expert", 0, 0, axis_index_groups=groups, tiled=True
        )

    a_far = swap(a_tokens)
    b_far = swap(b_cot)
    a_slot, a_gate = routing(a_ids, a_gates, a_valid, experts, capacity)
    b_slot, b_gate = routing(b_ids, b_gates, b_valid, experts, capacity)
    packed = jnp.stack([a_slot, a_gate, b_slot, b_gate])

    def take(x, which):
        return lax.dynamic_slice_in_dim(x, which * half, half, axis=x.ndim - 1)

    mine = take(packed, side)
    theirs = swap(take(packed, 1 - side))

    def both(x, y):
        x = x.reshape(half, 1, capacity, width)
        y = y.reshape(half, 1, capacity, width)
        return jnp.concatenate([x, y], axis=1).astype(jnp.bfloat16)

    a_send = both(
        pick(mine[0], a_tokens, capacity), pick(theirs[0], a_far, capacity)
    )
    rows = spread(a_send).reshape(-1, width)
    gate_proj = jnp.dot(rows, w_gate[0], preferred_element_type=jnp.float32)
    up_proj = jnp.dot(rows, w_up[0], preferred_element_type=jnp.float32)
    hidden = (jax.nn.silu(gate_proj) * up_proj).astype(jnp.bfloat16)
    made = jnp.dot(hidden, w_down[0], preferred_element_type=jnp.float32)
    made = made.astype(jnp.bfloat16).reshape(half, 2, capacity, width)
    back = spread(made)
    far_sum = combine(theirs[0], theirs[1], back[:, 1].reshape(-1, width), capacity)
    far_back = swap(far_sum.astype(jnp.bfloat16))
    near_sum = combine(mine[0], mine[1], back[:, 0].reshape(-1, width), capacity)
    a_out = (near_sum + far_back.astype(jnp.float32)).astype(jnp.bfloat16)

    b_send = both(
        pick_gated(mine[2], mine[3], b_cot, capacity),
        pick_gated(theirs[2], theirs[3], b_far, capacity),
    )
    b_rows = spread(b_send)
    held = b_hidden[0].reshape(2, half, capacity, -1)
    near_h = lax.dynamic_index_in_dim(held, side, 0, False)
    far_h = lax.dynamic_index_in_dim(held, 1 - side, 0, False)
    h_rows = jnp.stack([near_h, far_h], axis=1).reshape(-1, b_hidden.shape[2])
    b_rows = b_rows.reshape(-1, width)
    piece = width // replicas
    if replicas == 2:
        r = lax.axis_index("replica")

        def grad_of(which):
            cols = lax.dynamic_slice_in_dim(b_rows, which * piece, piece, axis=1)
            g = jnp.dot(h_rows.T, cols, preferred_element_type=jnp.float32)
            return g.astype(jnp.bfloat16)

        other = lax.ppermute(grad_of(1 - r), "replica", [(0, 1), (1, 0)])
        gradient = grad_of(r).astype(jnp.float32) + other.astype(jnp.float32)
    else:
        g = jnp.dot(h_rows.T, b_rows, preferred_element_type=jnp.float32)
        g = g.astype(jnp.bfloat16).reshape(-1, replicas, piece).swapaxes(0, 1)
        g = lax.all_to_all(g, "replica", 0, 0, tiled=True)
        gradient = jnp.sum(g.astype(jnp.float32), axis=0)
    return (a_out, gradient[None])


def solution(mesh):
    tokens = P(("expert", "replica"), None)
    flags = P(("expert", "replica"))
    held = P("expert", None, None)
    return jax.shard_map(
        body,
        mesh=mesh,
        in_specs=(tokens, tokens, tokens, flags) * 2
        + (P("expert", "replica", None), held, held, held),
        out_specs=(tokens, P("expert", None, "replica")),
        check_vma=False,
    )
```

```python
import functools

import jax
import jax.numpy as jnp
from jax import lax
from jax.experimental import pallas as pl
from jax.experimental.pallas import tpu as pltpu
from jax.sharding import PartitionSpec as P


F32 = jnp.float32
BF16 = jnp.bfloat16


LIMIT = 20 * 1024 * 1024


def call(kernel, outs, operands, flops, scalars=(), far=False, scratch=()):
    size = sum(x.size * x.dtype.itemsize for x in (*operands, *outs))
    space = pltpu.HBM if far else pltpu.VMEM
    if far:
        operands = [pltpu.with_memory_space_constraint(x, space) for x in operands]
    return pl.pallas_call(
        kernel,
        out_shape=[pltpu.VMEM(x.shape, x.dtype) for x in outs],
        in_specs=[pl.BlockSpec(memory_space=pltpu.SMEM)] * len(scalars)
        + [pl.BlockSpec(memory_space=space)] * len(operands),
        out_specs=[pl.BlockSpec(memory_space=pltpu.VMEM)] * len(outs),
        scratch_shapes=list(scratch),
        compiler_params=pltpu.CompilerParams(vmem_limit_bytes=LIMIT),
        cost_estimate=pl.CostEstimate(
            flops=flops, bytes_accessed=size, transcendentals=0
        ),
    )(*scalars, *operands)


def pieces(width):
    piece = 512 if width % 512 == 0 else width
    return [slice(at, at + piece) for at in range(0, width, piece)]


def own_kernel(capacity, plane, unit, me_ref, *refs):
    far, out_ref = refs[:8], refs[8]
    outs, near, sems = refs[9 : 9 + plane], refs[9 + plane : -1], refs[-1]
    copies = [
        pltpu.make_async_copy(src, dst, sems.at[n])
        for n, (src, dst) in enumerate(zip(far, near))
    ]
    for copy in copies:
        copy.start()
    for copy in copies[:6]:
        copy.wait()
    top, count = near[0].shape
    experts = out_ref.shape[0] // 4
    row = lax.broadcasted_iota(jnp.int32, (count, count), 0)
    col = lax.broadcasted_iota(jnp.int32, (count, count), 1)
    before = jnp.where(row < col, 1.0, 0.0).astype(BF16)
    which = lax.broadcasted_iota(jnp.int32, (experts, count), 0)
    for side in range(2):
        ids_ref, gates_ref, valid_ref = near[3 * side : 3 * side + 3]
        hit = jnp.zeros((experts, count), F32)
        gate = jnp.zeros((experts, count), F32)
        for k in range(top):
            match = ids_ref[k : k + 1, :] == which
            hit = jnp.where(match, 1.0, hit)
            gate = jnp.where(match, gates_ref[k : k + 1, :], gate)
        hit = jnp.where(valid_ref[...] > 0, hit, 0.0)
        earlier = jnp.dot(hit.astype(BF16), before, preferred_element_type=F32)
        slot = jnp.where((hit > 0.0) & (earlier < capacity), earlier, -1.0)
        out_ref[2 * side * experts : (2 * side + 1) * experts, :] = slot
        out_ref[(2 * side + 1) * experts : (2 * side + 2) * experts, :] = gate
    for copy in copies[6:]:
        copy.wait()
    pick_kernel(plane, unit, [0, 1], me_ref, out_ref, out_ref, *near[6:], *outs)


def start(me, small, tokens, experts, capacity, plane, unit):
    count, width = tokens[0].shape
    arrays = [*small, *tokens]
    outs = [jax.ShapeDtypeStruct((4 * experts, count), F32)]
    outs += [jax.ShapeDtypeStruct((2 * unit, width), BF16)] * plane
    return call(
        functools.partial(own_kernel, capacity, plane, unit),
        outs,
        arrays,
        1 << 22,
        [me],
        far=True,
        scratch=[pltpu.VMEM(x.shape, x.dtype) for x in arrays]
        + [pltpu.SemaphoreType.DMA((len(arrays),))],
    )


def load_kernel(count, *refs):
    copies = [
        pltpu.make_async_copy(refs[n], refs[count + n], refs[-1].at[n])
        for n in range(count)
    ]
    for copy in copies:
        copy.start()
    for copy in copies:
        copy.wait()


def load(arrays):
    return call(
        functools.partial(load_kernel, len(arrays)),
        [jax.ShapeDtypeStruct(x.shape, x.dtype) for x in arrays],
        arrays,
        1 << 28,
        far=True,
        scratch=[pltpu.SemaphoreType.DMA((len(arrays),))],
    )


def held_kernel(unit, capacity, places, at_ref, hidden_ref, out_ref):
    slots = hidden_ref.shape[1]
    row = lax.broadcasted_iota(jnp.int32, (unit, slots), 0)
    col = lax.broadcasted_iota(jnp.int32, (unit, slots), 1)
    order = [
        jnp.where((row + (at_ref[0] ^ e) * capacity == col) & (row < capacity), 1.0, 0.0)
        for e in places
    ]
    dims = (((1,), (1,)), ((), ()))
    out_ref[...] = lax.dot_general(
        hidden_ref[...], join(order, 0).astype(BF16), dims, preferred_element_type=F32
    ).astype(BF16)


def matches(me, plane, unit, sides, metas):
    experts, count = metas[0].shape[0] // 4, metas[0].shape[1]
    at = lax.broadcasted_iota(jnp.int32, (len(metas) * unit, count), 0).astype(F32)
    found = []
    for q in range(plane):
        hit, gate = [], []
        for n, (side, meta) in enumerate(zip(sides, metas)):
            slot = meta[pl.ds((2 * side * experts + me) ^ q, 1), :]
            hit.append((slot == at - float(n * unit)) & (slot >= 0.0))
            gate.append(meta[pl.ds(((2 * side + 1) * experts + me) ^ q, 1), :])
        found.append((hit, gate))
    return found


def join(xs, axis):
    return jnp.concatenate(xs, axis=axis) if len(xs) > 1 else xs[0]


def pick_kernel(plane, unit, sides, me_ref, *refs):
    blocks = len(sides)
    metas, tokens, outs = refs[:blocks], refs[blocks : 2 * blocks], refs[2 * blocks :]
    rows = blocks * unit
    found = matches(me_ref[0], plane, unit, sides, metas)
    one = join(
        [join([jnp.where(h, 1.0, 0.0) for h in hit], 1) for hit, _ in found], 0
    ).astype(BF16)
    scale = [
        sum(
            jnp.sum(jnp.where(h, g if side else 1.0, 0.0), axis=1, keepdims=True)
            for side, h, g in zip(sides, hit, gate)
        )
        for hit, gate in found
    ]
    for cols in pieces(tokens[0].shape[1]):
        held = join([t[:, cols] for t in tokens], 0)
        got = jnp.dot(one, held, preferred_element_type=F32)
        for q in range(plane):
            piece = got[q * rows : (q + 1) * rows]
            if any(sides):
                piece *= scale[q]
            outs[q][:, cols] = piece.astype(BF16)


def pick(me, plane, unit, sides, metas, tokens):
    blocks, (count, width) = len(tokens), tokens[0].shape
    out = jax.ShapeDtypeStruct((blocks * unit, width), BF16)
    return call(
        functools.partial(pick_kernel, plane, unit, sides),
        [out] * plane,
        [*metas, *tokens],
        2 * plane * blocks * unit * blocks * count * width,
        [me],
    )


def combine_kernel(plane, unit, blocks, added, me_ref, *refs):
    metas, parts = refs[:blocks], refs[blocks : blocks + plane]
    extra, outs = refs[blocks + plane :][:added], refs[blocks + plane + added :]
    count = outs[0].shape[0]
    found = matches(me_ref[0], plane, unit, [0] * blocks, metas)
    coef = join(
        [
            join([jnp.where(h, g, 0.0) for h, g in zip(hit, gate)], 1)
            for hit, gate in found
        ],
        0,
    )
    high = coef.astype(BF16)
    low = (coef - high.astype(F32)).astype(BF16)
    dims = (((0,), (0,)), ((), ()))
    for cols in pieces(parts[0].shape[1]):
        held = join([p[:, cols] for p in parts], 0)
        got = lax.dot_general(high, held, dims, preferred_element_type=F32)
        got += lax.dot_general(low, held, dims, preferred_element_type=F32)
        for n, out in enumerate(outs):
            total = got[n * count : (n + 1) * count]
            if added:
                total += extra[n][:, cols].astype(F32)
            out[:, cols] = total.astype(out.dtype)


def combine(me, unit, metas, parts, types, extra=()):
    plane, (rows, width) = len(parts), parts[0].shape
    count = metas[0].shape[1]
    return call(
        functools.partial(combine_kernel, plane, unit, len(metas), len(extra)),
        [jax.ShapeDtypeStruct((count, width), t) for t in types],
        [*metas, *parts, *extra],
        4 * plane * rows * len(metas) * count * width,
        [me],
    )


def ffn_kernel(plane, unit, takes, gives, *refs):
    groups = len(takes)
    parts = refs[: plane * groups]
    gate_ref, up_ref, down_ref = refs[plane * groups : plane * groups + 3]
    outs = refs[plane * groups + 3 :]
    x = join(
        [
            parts[g * plane + q][: blocks * unit]
            for q in range(plane)
            for g, blocks in enumerate(takes)
        ],
        0,
    )
    total = sum(takes)
    dims = (((1,), (1,)), ((), ()))
    gate = lax.dot_general(x, gate_ref[...], dims, preferred_element_type=F32)
    up = lax.dot_general(x, up_ref[...], dims, preferred_element_type=F32)
    hidden = (gate / (1.0 + jnp.exp(-gate)) * up).astype(BF16)
    for cols in pieces(down_ref.shape[1]):
        y = jnp.dot(hidden, down_ref[:, cols], preferred_element_type=F32)
        for q in range(plane):
            at = q * total * unit
            for n, blocks in enumerate(gives):
                rows = blocks * unit
                outs[n * plane + q][:, cols] = y[at : at + rows].astype(BF16)
                at += rows


def ffn(unit, groups, takes, gives, weights):
    plane, width = len(groups[0]), groups[0][0].shape[1]
    made = call(
        functools.partial(ffn_kernel, plane, unit, takes, gives),
        [
            jax.ShapeDtypeStruct((blocks * unit, width), BF16)
            for blocks in gives
            for _ in range(plane)
        ],
        [*(p for parts in groups for p in parts), *weights],
        6 * plane * sum(takes) * unit * width * weights[0].shape[0],
    )
    return [made[n * plane : (n + 1) * plane] for n in range(len(gives))]


def grad_kernel(starts, at_ref, held_ref, *refs):
    parts, out = refs[:-1], refs[-1]
    piece = out.shape[1]
    cols = pl.ds(pl.multiple_of(at_ref[0] * piece, 128), piece)
    rows = join([p[start:, cols] for p, start in zip(parts, starts)], 0)
    out[...] = jnp.dot(held_ref[...], rows, preferred_element_type=F32).astype(BF16)


def grad(at, held, parts, starts, piece):
    inner, slots = held.shape
    return call(
        functools.partial(grad_kernel, starts),
        [jax.ShapeDtypeStruct((inner, piece), BF16)],
        [held, *parts],
        2 * inner * slots * piece,
        [at],
    )[0]


def body(
    a_tokens,
    a_ids,
    a_gates,
    a_valid,
    b_cot,
    b_ids,
    b_gates,
    b_valid,
    b_hidden,
    w_gate,
    w_up,
    w_down,
):
    experts = lax.axis_size("expert")
    replicas = lax.axis_size("replica")
    capacity = b_hidden.shape[1] // experts
    _, width = a_tokens.shape
    bits = experts.bit_length() - 1
    plane = 1 << ((bits + 1) // 2)
    unit = -(-capacity // 8) * 8
    layers = experts // plane
    index = lax.axis_index("expert")
    me = jnp.full((1,), index, jnp.int32)
    strides = []
    s = layers // 4
    while s:
        strides.append(s)
        s //= 2
    far_stride = layers // 2

    def swap(x, mask):
        return lax.ppermute(
            x, "expert", [(e, e ^ mask) for e in range(experts)]
        )

    def gather(first, offset, steps=strides):
        have = [(offset, first)]
        for s in steps:
            have += [(j + s, swap(x, s * plane)) for j, x in have]
        return sorted(have, key=lambda pair: pair[0])

    def fold(sums, steps):
        for s in reversed(steps):
            sent = {j ^ s: swap(x, s * plane) for j, x in sums.items() if j & s}
            sums = {
                j: (x.astype(F32) + sent[j].astype(F32)).astype(x.dtype)
                for j, x in sums.items()
                if not j & s
            }
        return sums

    def deliver(parts):
        steps = sorted(range(1, len(parts)), key=lambda q: q.bit_count())
        moved = {q: swap(parts[q], q) for q in steps}
        return [parts[0]] + [moved[q] for q in range(1, len(parts))]

    a_near = gather(a_tokens, 0)
    a_across = swap(a_tokens, far_stride * plane)
    small = [a_ids.T, a_gates.T, a_valid[None], b_ids.T, b_gates.T, b_valid[None]]
    meta, *own = start(
        me, small, [a_tokens, b_cot], experts, capacity, plane, unit
    )
    weights = load([w_gate[0].T, w_up[0].T, w_down[0]])
    metas = [meta] + [swap(meta, j * plane) for j in range(1, layers)]

    def send(*items):
        sides = [side for side, _, _ in items]
        known = [metas[j] for _, j, _ in items]
        tokens = [x for _, _, x in items]
        sends = pick(me, plane, unit, sides, known, tokens)
        return deliver(sends)

    def back(blocks, parts, extra=()):
        known = [metas[j] for j in blocks]
        types = [F32 if j == 0 else BF16 for j in blocks]
        parts = deliver(parts)
        sums = combine(me, unit, known, parts, types, extra)
        return dict(zip(blocks, sums))

    a_far = gather(a_across, far_stride)
    last = strides[-1]
    mid = [(0, j, x) for j, x in a_far if not j & last]
    end = [(0, j, x) for j, x in a_far if j & last]
    near = [(0, j, x) for j, x in a_near if j]
    own = deliver(own)
    middle = send(*near, *mid)
    final = send(*end)
    near_out, mid_out = ffn(
        unit,
        [own, middle],
        [1, len(near) + len(mid)],
        [1 + len(near), len(mid)],
        weights,
    )
    (end_out,) = ffn(unit, [final], [len(end)], [len(end)], weights)
    late = back([j for _, j, _ in end], end_out)
    came = [swap(late[j ^ last], last * plane) for _, j, _ in mid]
    far = back([j for _, j, _ in mid], mid_out, came)
    near_sum = back([0] + [j for _, j, _ in near], near_out)
    far = fold(far, strides[:-1])
    far_back = swap(far[far_stride], far_stride * plane)
    near_sum = fold(near_sum, strides)

    b_across = swap(b_cot, far_stride * plane)
    b_have = gather(b_cot, 0) + gather(b_across, far_stride)
    b_have = [(1, j, x) for j, x in b_have if j]
    b_parts = own + send(*b_have)
    starts = [unit] * plane + [0] * plane
    places = list(range(plane))
    places += [j * plane + q for q in range(plane) for _, j, _ in b_have]
    held = call(
        functools.partial(held_kernel, unit, capacity, places),
        [jax.ShapeDtypeStruct((b_hidden.shape[2], experts * unit), BF16)],
        [b_hidden[0].T],
        2 * b_hidden.shape[2] * b_hidden.shape[1] * experts * unit,
        [me],
    )[0]
    piece = width // replicas
    mine = lax.axis_index("replica")
    others = []
    for s in range(1, replicas):
        at = jnp.full((1,), mine ^ s, jnp.int32)
        pairs = [(k, k ^ s) for k in range(replicas)]
        part = grad(at, held, b_parts, starts, piece)
        others.append(lax.ppermute(part, "replica", pairs))
    at = jnp.full((1,), mine, jnp.int32)
    gradient = grad(at, held, b_parts, starts, piece)
    gradient = gradient.astype(F32)
    for x in others:
        gradient += x.astype(F32)
    far_back, gradient = lax.optimization_barrier((far_back, gradient))
    a_out = (near_sum[0] + far_back.astype(F32)).astype(BF16)
    return (a_out, gradient[None])


def solution(mesh):
    tokens = P(("expert", "replica"), None)
    flags = P(("expert", "replica"))
    held = P("expert", None, None)
    return jax.shard_map(
        body,
        mesh=mesh,
        in_specs=(tokens, tokens, tokens, flags) * 2
        + (P("expert", "replica", None), held, held, held),
        out_specs=(tokens, P("expert", None, "replica")),
        check_vma=False,
    )
```
